32 devices in a mesh: tm: 4 (over y, x), paths: 8 (over z, core).
Axes of the slice: x: 2, y: 2, z: 4, core: 2. Of those that a mesh axis runs over, the one named last changes fastest.
Arguments:
- returns: bfloat16 [128, 4096, 256], P('tm', 'paths'), may hold values from -0.15917969 to 0.15917969
- weights: bfloat16 [256, 64], P('paths'), may hold values from -0.375 to 0.375
Outputs:
- drawdown: float32 [64, 4096], P('tm', 'paths')
The draws below stay inside these ranges and needn't reach their ends.
All inputs are finite; a program needn't handle non-finite values.
Results may differ from the reference program's by a relative error of at most 0.0003.
Values may be sent and summed in bfloat16 or wider, within the bound.
A program may use at most 64 MiB of HBM per device.

```python
import jax
import jax.numpy as jnp
from jax import lax

ASSETS = 256
PORT = 64
T_DEV = 32
STEPS = 128
PATHS = 4096
N_TM = 4


def block_levels(key, shape, shards, smallest, high):
    loudness = 1.0
    for dim, parts in shards:
        heights = jax.random.uniform(jax.random.fold_in(jax.random.fold_in(key, 6), dim), (parts,), jnp.float32, smallest / len(shards), high / len(shards))
        loudness = loudness * jnp.repeat(jnp.exp(heights), shape[dim] // parts).reshape((-1,) + (1,) * (len(shape) - 1 - dim))
    return loudness


def bell_draw(stream_key, dims, spread, limit, split=(), kind=jnp.bfloat16):
    loudness = block_levels(stream_key, dims, split, -0.22, 0.18) if split else 1.0
    array = jax.random.normal(stream_key, dims, jnp.float32) * spread * loudness
    return jnp.minimum(jnp.maximum(array, -limit), limit).astype(kind)


def setup_inputs(seed: int = 0) -> dict:
    keys = jax.random.split(jax.random.key(seed), 3)
    return {
        "returns": bell_draw(keys[0], (STEPS, PATHS, ASSETS), 0.02, 0.15917969, ((0, 4), (1, 8))),
        "weights": bell_draw(keys[1], (ASSETS, PORT), ASSETS ** -0.5, 0.375, ((0, 8),)),
    }


def reference(returns, weights):
    blocks = returns.reshape(N_TM, T_DEV, PATHS, ASSETS)
    holdings = weights.astype(jnp.float32)

    def advance(carry, block):
        level, highest, deepest = carry
        profit = jnp.einsum('tpa,aq->tqp', block.astype(jnp.float32), holdings)
        value = level[None] + jnp.cumsum(profit, axis=0)
        running = jnp.maximum(highest[None], lax.cummax(value, axis=0))
        deepest = jnp.maximum(deepest, jnp.max(running - value, axis=0))
        return (value[-1], running[-1], deepest), None

    zeros = jnp.zeros((PORT, PATHS), jnp.float32)
    final, unused = lax.scan(advance, (zeros, zeros, zeros), blocks)
    return final[2]
```

```python
import functools

import jax
import jax.numpy as jnp
from jax import lax
from jax.experimental import pallas as pl
from jax.experimental.pallas import tpu as pltpu
from jax.sharding import PartitionSpec as P

MESH = pl.DeviceIdType.MESH
CHUNKS = 2
GROUP = 8
ROWS = 32


def kernel(
    n_tm, n_paths, ret_hbm, w_ref, out_ref,
    ret, wbuf, prof, send, recv, load_sem, wsend_sem, wrecv_sem, send_sem, recv_sem,
):
    steps, paths, assets = ret.shape
    ports = w_ref.shape[1]
    block = ports // n_tm
    width = paths // CHUNKS
    half = width // 2
    groups = steps // GROUP
    tm = lax.axis_index("tm")
    me = lax.axis_index("paths")

    def load(c, g):
        part = (pl.ds(g * GROUP, GROUP), pl.ds(c * width, width))
        return pltpu.make_async_copy(ret_hbm.at[part], ret.at[part], load_sem.at[c, g])

    for c in range(CHUNKS):
        for g in range(groups):
            load(c, g).start()

    barrier = pltpu.get_barrier_semaphore()
    for d in range(1, n_paths):
        pl.semaphore_signal(
            barrier, inc=1, device_id=(tm, lax.rem(me + d, n_paths)), device_id_type=MESH
        )
    for d in range(1, n_tm):
        pl.semaphore_signal(
            barrier, inc=1, device_id=(lax.rem(tm + d, n_tm), me), device_id_type=MESH
        )
    pl.semaphore_wait(barrier, n_paths - 1 + n_tm - 1)

    def weight_copy(d):
        return pltpu.make_async_remote_copy(
            src_ref=w_ref,
            dst_ref=wbuf.at[me],
            send_sem=wsend_sem.at[d - 1],
            recv_sem=wrecv_sem.at[d - 1],
            device_id=(tm, lax.rem(me + d, n_paths)),
            device_id_type=MESH,
        )

    def weight_arrival(d):
        return pltpu.make_async_remote_copy(
            src_ref=w_ref,
            dst_ref=wbuf.at[lax.rem(me + n_paths - d, n_paths)],
            send_sem=wsend_sem.at[d - 1],
            recv_sem=wrecv_sem.at[d - 1],
            device_id=(tm, lax.rem(me + d, n_paths)),
            device_id_type=MESH,
        )

    for d in range(1, n_paths):
        weight_copy(d).start()
    wbuf[me] = w_ref[...]
    for d in range(1, n_paths):
        weight_arrival(d).wait_recv()

    held = wbuf[...].reshape(assets, ports)
    blank = jnp.zeros_like(held)
    both = jnp.concatenate(
        [jnp.concatenate([held, blank], axis=1), jnp.concatenate([blank, held], axis=1)], axis=0
    )

    def block_copy(c, d, slot):
        return pltpu.make_async_remote_copy(
            src_ref=send.at[c, lax.rem(tm + d, n_tm)],
            dst_ref=recv.at[c, slot],
            send_sem=send_sem.at[c, d - 1],
            recv_sem=recv_sem.at[c, d - 1],
            device_id=(lax.rem(tm + d, n_tm), me),
            device_id_type=MESH,
        )

    for c in range(CHUNKS):
        first = pl.ds(c * width, half)
        second = pl.ds(c * width + half, half)
        for g in range(groups):
            load(c, g).wait()
            when = pl.ds(g * GROUP, GROUP)
            left = ret[when, first, :].reshape(GROUP * half, assets)
            right = ret[when, second, :].reshape(GROUP * half, assets)
            prof[c, when] = jnp.dot(
                jnp.concatenate([left, right], axis=1), both, preferred_element_type=jnp.float32
            ).reshape(GROUP, half, 2 * ports)
        pieces = []
        for r in range(0, half, ROWS):
            value = prof[c, 0, pl.ds(r, ROWS)]
            high, low, fall = value, value, jnp.zeros_like(value)
            for t in range(1, steps):
                value = value + prof[c, t, pl.ds(r, ROWS)]
                high = jnp.maximum(high, value)
                low = jnp.minimum(low, value)
                fall = jnp.maximum(fall, high - value)
            pieces.append((value, high, fall, low))
        for k in range(4):
            whole = jnp.concatenate([piece[k] for piece in pieces], axis=0).T
            for b in range(n_tm):
                rows = b * block
                send[c, b, k, :, 0:half] = whole[rows : rows + block]
                send[c, b, k, :, half:width] = whole[ports + rows : ports + rows + block]
        for d in range(1, n_tm):
            block_copy(c, d, tm).start()
        recv[c, tm] = send[c, tm]

    for c in range(CHUNKS):
        for d in range(1, n_tm):
            block_copy(c, d, lax.rem(tm + n_tm - d, n_tm)).wait_recv()
        level = jnp.zeros((block, width), jnp.float32)
        peak, deepest = level, level
        for s in range(n_tm):
            deepest = jnp.maximum(deepest, recv[c, s, 2])
            deepest = jnp.maximum(deepest, peak - (level + recv[c, s, 3]))
            peak = jnp.maximum(peak, level + recv[c, s, 1])
            level = level + recv[c, s, 0]
        out_ref[:, pl.ds(c * width, width)] = deepest

    for d in range(1, n_paths):
        weight_copy(d).wait_send()
    for c in range(CHUNKS):
        for d in range(1, n_tm):
            block_copy(c, d, tm).wait_send()


def solution(mesh):
    n_tm, n_paths = mesh.shape["tm"], mesh.shape["paths"]

    def shards(returns, weights):
        steps, paths, assets = returns.shape
        share, ports = weights.shape
        block, width = ports // n_tm, paths // CHUNKS
        dma = pltpu.SemaphoreType.DMA
        return pl.pallas_call(
            functools.partial(kernel, n_tm, n_paths),
            out_shape=jax.ShapeDtypeStruct((block, paths), jnp.float32),
            in_specs=[
                pl.BlockSpec(memory_space=pl.ANY),
                pl.BlockSpec(memory_space=pltpu.VMEM),
            ],
            out_specs=pl.BlockSpec(memory_space=pltpu.VMEM),
            scratch_shapes=[
                pltpu.VMEM((steps, paths, assets), returns.dtype),
                pltpu.VMEM((n_paths, share, ports), weights.dtype),
                pltpu.VMEM((CHUNKS, steps, width // 2, 2 * ports), jnp.float32),
                pltpu.VMEM((CHUNKS, n_tm, 4, block, width), jnp.float32),
                pltpu.VMEM((CHUNKS, n_tm, 4, block, width), jnp.float32),
                dma((CHUNKS, steps // GROUP)),
                dma((n_paths - 1,)),
                dma((n_paths - 1,)),
                dma((CHUNKS, n_tm - 1)),
                dma((CHUNKS, n_tm - 1)),
            ],
            compiler_params=pltpu.CompilerParams(
                collective_id=0, has_side_effects=True, vmem_limit_bytes=40 << 20
            ),
        )(returns, weights)

    in_specs = (P("tm", "paths", None), P("paths", None))
    out_specs = P("tm", "paths")
    return jax.shard_map(shards, mesh=mesh, in_specs=in_specs, out_specs=out_specs, check_vma=False)
```

```python
import functools

import jax
import jax.numpy as jnp
from jax import lax
from jax.experimental import pallas as pl
from jax.experimental.pallas import tpu as pltpu
from jax.sharding import PartitionSpec as P

MESH = pl.DeviceIdType.MESH
CHUNKS = 2
ROWS = 32


def kernel(
    n_tm, n_paths, ret_hbm, w_hbm, out_ref,
    ret, w_ref, wbuf, prof, send, recv, load_sem, own_sem, wsend_sem, wrecv_sem, send_sem, recv_sem,
):
    steps, paths, assets = ret.shape
    ports = w_ref.shape[1]
    block = ports // n_tm
    width = paths // CHUNKS
    half = width // 2
    groups = 1
    tm = lax.axis_index("tm")
    me = lax.axis_index("paths")

    def load(c, g):
        part = (pl.ds(g * steps, steps), pl.ds(c * width, width))
        return pltpu.make_async_copy(ret_hbm.at[part], ret.at[part], load_sem.at[c, g])

    own = pltpu.make_async_copy(w_hbm, w_ref, own_sem)
    own.start()
    for c in range(CHUNKS):
        for g in range(groups):
            load(c, g).start()

    barrier = pltpu.get_barrier_semaphore()
    for d in range(1, n_paths):
        pl.semaphore_signal(
            barrier, inc=1, device_id=(tm, lax.rem(me + d, n_paths)), device_id_type=MESH
        )
    for d in range(1, n_tm):
        pl.semaphore_signal(
            barrier, inc=1, device_id=(lax.rem(tm + d, n_tm), me), device_id_type=MESH
        )
    own.wait()
    pl.semaphore_wait(barrier, n_paths - 1 + n_tm - 1)

    def weight_copy(d):
        return pltpu.make_async_remote_copy(
            src_ref=w_ref,
            dst_ref=wbuf.at[me],
            send_sem=wsend_sem.at[d - 1],
            recv_sem=wrecv_sem.at[d - 1],
            device_id=(tm, lax.rem(me + d, n_paths)),
            device_id_type=MESH,
        )

    def weight_arrival(d):
        return pltpu.make_async_remote_copy(
            src_ref=w_ref,
            dst_ref=wbuf.at[lax.rem(me + n_paths - d, n_paths)],
            send_sem=wsend_sem.at[d - 1],
            recv_sem=wrecv_sem.at[d - 1],
            device_id=(tm, lax.rem(me + d, n_paths)),
            device_id_type=MESH,
        )

    for d in range(1, n_paths):
        weight_copy(d).start()
    wbuf[me] = w_ref[...]
    for d in range(1, n_paths):
        weight_arrival(d).wait_recv()

    held = wbuf[...].reshape(assets, ports)
    blank = jnp.zeros_like(held)
    both = jnp.concatenate(
        [jnp.concatenate([held, blank], axis=1), jnp.concatenate([blank, held], axis=1)], axis=0
    )

    def block_copy(c, d, slot):
        return pltpu.make_async_remote_copy(
            src_ref=send.at[c, lax.rem(tm + d, n_tm)],
            dst_ref=recv.at[c, slot],
            send_sem=send_sem.at[c, d - 1],
            recv_sem=recv_sem.at[c, d - 1],
            device_id=(lax.rem(tm + d, n_tm), me),
            device_id_type=MESH,
        )

    for c in range(CHUNKS):
        first = pl.ds(c * width, half)
        second = pl.ds(c * width + half, half)
        for g in range(groups):
            load(c, g).wait()
            when = pl.ds(g * steps, steps)
            left = ret[when, first, :].reshape(steps * half, assets)
            right = ret[when, second, :].reshape(steps * half, assets)
            prof[c, when] = jnp.dot(
                jnp.concatenate([left, right], axis=1), both, preferred_element_type=jnp.float32
            ).reshape(steps, half, 2 * ports)
        pieces = []
        for r in range(0, half, ROWS):
            value = prof[c, 0, pl.ds(r, ROWS)]
            high, low, fall = value, value, jnp.zeros_like(value)
            for t in range(1, steps):
                value = value + prof[c, t, pl.ds(r, ROWS)]
                high = jnp.maximum(high, value)
                low = jnp.minimum(low, value)
                fall = jnp.maximum(fall, high - value)
            pieces.append((value, high, fall, low))
        for k in range(4):
            whole = jnp.concatenate([piece[k] for piece in pieces], axis=0).T
            for b in range(n_tm):
                rows = b * block
                send[c, b, k, :, 0:half] = whole[rows : rows + block]
                send[c, b, k, :, half:width] = whole[ports + rows : ports + rows + block]
        for d in range(1, n_tm):
            block_copy(c, d, tm).start()
        recv[c, tm] = send[c, tm]

    for c in range(CHUNKS):
        for d in range(1, n_tm):
            block_copy(c, d, lax.rem(tm + n_tm - d, n_tm)).wait_recv()
        level = jnp.zeros((block, width), jnp.float32)
        peak, deepest = level, level
        for s in range(n_tm):
            deepest = jnp.maximum(deepest, recv[c, s, 2])
            deepest = jnp.maximum(deepest, peak - (level + recv[c, s, 3]))
            peak = jnp.maximum(peak, level + recv[c, s, 1])
            level = level + recv[c, s, 0]
        out_ref[:, pl.ds(c * width, width)] = deepest

    for d in range(1, n_paths):
        weight_copy(d).wait_send()
    for c in range(CHUNKS):
        for d in range(1, n_tm):
            block_copy(c, d, tm).wait_send()


def solution(mesh):
    n_tm, n_paths = mesh.shape["tm"], mesh.shape["paths"]

    def shards(returns, weights):
        steps, paths, assets = returns.shape
        share, ports = weights.shape
        block, width = ports // n_tm, paths // CHUNKS
        dma = pltpu.SemaphoreType.DMA
        return pl.pallas_call(
            functools.partial(kernel, n_tm, n_paths),
            out_shape=jax.ShapeDtypeStruct((block, paths), jnp.float32),
            in_specs=[
                pl.BlockSpec(memory_space=pltpu.HBM),
                pl.BlockSpec(memory_space=pltpu.HBM),
            ],
            out_specs=pl.BlockSpec(memory_space=pltpu.VMEM),
            scratch_shapes=[
                pltpu.VMEM((steps, paths, assets), returns.dtype),
                pltpu.VMEM((share, ports), weights.dtype),
                pltpu.VMEM((n_paths, share, ports), weights.dtype),
                pltpu.VMEM((CHUNKS, steps, width // 2, 2 * ports), jnp.float32),
                pltpu.VMEM((CHUNKS, n_tm, 4, block, width), jnp.float32),
                pltpu.VMEM((CHUNKS, n_tm, 4, block, width), jnp.float32),
                dma((CHUNKS, 1)),
                dma,
                dma((n_paths - 1,)),
                dma((n_paths - 1,)),
                dma((CHUNKS, n_tm - 1)),
                dma((CHUNKS, n_tm - 1)),
            ],
            compiler_params=pltpu.CompilerParams(
                collective_id=0, has_side_effects=True, vmem_limit_bytes=63 << 20
            ),
        )(returns, weights)

    in_specs = (P("tm", "paths", None), P("paths", None))
    out_specs = P("tm", "paths")
    return jax.shard_map(shards, mesh=mesh, in_specs=in_specs, out_specs=out_specs, check_vma=False)
```
